32 devices in a mesh: row: 4 (over y, x), col: 8 (over z, core).
Axes of the slice: x: 2, y: 2, z: 4, core: 2. Of those that a mesh axis runs over, the one named last changes fastest.
Arguments:
- adjacency: int32 [8192, 256], P('row', 'col'), may hold values from -2147483648 to 2147483647, as said below
- seed_mask: int32 [8192], P('col'), may hold values 0 or 1
- source: int32 [1], replicated, may hold values from 0 to 8191
Outputs:
- levels: int32 [8192], P('col')
- parents: int32 [8192], P('col')
The draws below stay inside these ranges and needn't reach their ends.
Inputs may be any that keep to these rules, and one draw needn't show every extreme that they name: adjacency is symmetric (edge(u, v) = edge(v, u)); it is the union of 131072 Kronecker edges whose endpoints pick one of four quadrants per bit with weights 57, 19, 19, 5 out of 100, vertex labels not permuted, so low ids carry most edges; each word is a 32-bit pattern read as a signed int32.
All inputs are finite; a program needn't handle non-finite values.
Results may differ from the reference program's by a relative error of at most 0.000001.
Values may be sent and summed in bfloat16 or wider, within the bound.
A program may use at most 64 MiB of HBM per device.

```python
import math
import jax
import jax.numpy as jnp
from jax import lax

LEVELS = 4
EDGES = 16
V = 8192


def draw_adjacency(key, part):
    vertex_total = V
    bit_count = max((vertex_total - 1).bit_length(), 1)
    edge_total = EDGES * vertex_total
    sources = jnp.zeros((edge_total,), jnp.int32)
    targets = jnp.zeros((edge_total,), jnp.int32)
    for bit_no in range(bit_count):
        quadrant = jax.random.randint(jax.random.fold_in(key, 11 + bit_no), (edge_total,), 0, 100, dtype=jnp.int32)
        high_src = (quadrant >= 76).astype(jnp.int32)
        high_dst = ((quadrant >= 57) & (quadrant < 76) | (quadrant >= 95)).astype(jnp.int32)
        sources = sources * 2 + high_src
        targets = targets * 2 + high_dst
    sources = sources % vertex_total
    targets = targets % vertex_total
    ends_first = jnp.concatenate([sources, targets])
    ends_second = jnp.concatenate([targets, sources])
    word_count = vertex_total // 32
    word_key = (ends_first * word_count + ends_second // 32).astype(jnp.int32)
    bit_pos = (ends_second % 32).astype(jnp.int32)
    word_sorted, bit_sorted = lax.sort((word_key, bit_pos), num_keys=2)
    changed = (word_sorted[1:] != word_sorted[:-1]) | (bit_sorted[1:] != bit_sorted[:-1])
    distinct = jnp.concatenate([jnp.ones((1,), bool), changed])
    weights = jnp.where(distinct, jnp.left_shift(jnp.int32(1), bit_sorted), 0).astype(jnp.int32)
    packed = jax.ops.segment_sum(weights, word_sorted, num_segments=vertex_total * word_count)
    return packed.astype(jnp.int32).reshape(vertex_total, word_count)


def touch_ends(drawn, key, smallest, largest):
    longest = drawn.shape.index(max(drawn.shape))
    spots = []
    for shift in (0, 1):
        where = [jax.random.randint(jax.random.fold_in(key, axis), (), 0, length) for axis, length in enumerate(drawn.shape)]
        where[longest] = (where[longest] + shift) % drawn.shape[longest]
        spots.append(tuple(where))
    return drawn.at[spots[0]].set(smallest).at[spots[1]].set(largest)


def setup_inputs(seed: int = 0) -> dict:
    arg_keys = jax.random.split(jax.random.key(seed), 4)
    adjacency = draw_adjacency(jax.random.fold_in(arg_keys[3], 71), 0)
    seed_mask = touch_ends((jax.random.randint(arg_keys[1], (V,), 0, V // 4) < 1).astype(jnp.int32), jax.random.fold_in(arg_keys[1], 1), 0, 1)
    source = jax.random.randint(arg_keys[2], (1,), 0, V).astype(jnp.int32)
    return dict(adjacency=adjacency, seed_mask=seed_mask, source=source)


absent = 1073741824


def unpack(words):
    shifts = jnp.arange(32, dtype=jnp.int32)
    bit_table = jnp.bitwise_and(jnp.right_shift(words[..., None], shifts), 1)
    return bit_table.reshape(words.shape[:-1] + (words.shape[-1] * 32,))


def nearest_sources(adjacency, active, first_row):
    height = adjacency.shape[0]
    width = adjacency.shape[1] * 32
    block_rows = math.gcd(height, 256)

    def sweep_block(lowest, block_id):
        offset = block_id * block_rows
        tile_words = lax.dynamic_slice_in_dim(adjacency, offset, block_rows, 0)
        marks = lax.dynamic_slice_in_dim(active, offset, block_rows, 0)

        def scan_tile(current):
            row_ids = first_row + offset + jnp.arange(block_rows, dtype=jnp.int32)
            linked = (unpack(tile_words) * marks[:, None]) > 0
            found = jnp.min(jnp.where(linked, row_ids[:, None], absent), axis=0)
            return jnp.minimum(current, found)

        def keep_tile(current):
            return current

        lowest = lax.cond(jnp.any(marks > 0), scan_tile, keep_tile, lowest)
        return lowest, None

    start_value = jnp.full((width,), absent, jnp.int32)
    lowest, unused = lax.scan(sweep_block, start_value, jnp.arange(height // block_rows, dtype=jnp.int32))
    return lowest


def reference(adjacency, seed_mask, source):
    vertex_ids = jnp.arange(adjacency.shape[0], dtype=jnp.int32)
    reached = (seed_mask > 0) | (vertex_ids == source[0])
    levels = jnp.where(reached, 0, -1).astype(jnp.int32)
    parents = jnp.where(reached, vertex_ids, -1).astype(jnp.int32)
    frontier = reached.astype(jnp.int32)
    for depth_no in range(1, LEVELS + 1):
        nearest = nearest_sources(adjacency, frontier, jnp.int32(0))
        fresh = (nearest < absent) & (levels < 0)
        levels = jnp.where(fresh, depth_no, levels).astype(jnp.int32)
        parents = jnp.where(fresh, nearest, parents).astype(jnp.int32)
        frontier = fresh.astype(jnp.int32)
    return levels, parents
```

```python
import functools

import jax
import jax.numpy as jnp
from jax import lax
from jax.experimental import pallas as pl
from jax.experimental.pallas import tpu as pltpu
from jax.sharding import PartitionSpec as P

LEVELS = 4
MESH = pl.DeviceIdType.MESH
PAIR = 0x10001


def log2(n):
    return n.bit_length() - 1


def gather_lanes(x, idx):
    return jnp.take_along_axis(x, idx, axis=1)


def repeat(n, body, init):
    if n <= 4:
        for i in range(n):
            init = body(i, init)
        return init
    return lax.fori_loop(0, n, body, init)


def merge(low, high):
    rest = ~low[0]
    out = [low[0] | high[0]]
    for a, b in zip(low[1:], high[1:]):
        out.append(a | (b & rest))
    out.append(high[0] & rest)
    return out


def kernel(R, C, adj_ref, seed_ref, src_ref, lev_ref, par_ref,
           words_ref, col_buf, row_buf, key_buf,
           col_send, col_recv, row_send, row_recv, key_send, key_recv):
    me_r = lax.axis_index("row")
    me_c = lax.axis_index("col")
    height, wd = adj_ref.shape
    G = 128 // wd
    K = height // 256
    KG = K // G
    NB = 128 // K
    NTC = 16 // NB
    NTR = 4 // G
    total = R * height

    barrier = pltpu.get_barrier_semaphore()
    for step in range(1, C):
        pl.semaphore_signal(barrier, inc=1, device_id={"col": lax.rem(me_c + step, C)}, device_id_type=MESH)
    for step in range(1, R):
        pl.semaphore_signal(barrier, inc=1, device_id={"row": lax.rem(me_r + step, R)}, device_id_type=MESH)

    lane = lax.broadcasted_iota(jnp.int32, (8, 128), 1)
    sub = lax.broadcasted_iota(jnp.int32, (8, 128), 0)
    zero = jnp.zeros((8, 128), jnp.int32)

    leaves = height // 8 // G

    def compact(i, carry):
        for t in range(8):
            j = i * 8 + t
            parts = [adj_ref[pl.ds(g * leaves + j, 8, stride=height // 8), :] for g in range(G)]
            words_ref[j] = parts[0] if G == 1 else jnp.concatenate(parts, axis=1)
        return carry

    lax.fori_loop(0, leaves // 8, compact, 0)

    source = src_ref[0]
    first = me_c * (wd * 32)
    word_of = lane % wd
    words = zero
    for q in range(seed_ref.shape[0] // 8):
        vid = first + (sub + 8 * q) * 128 + lane
        x = jnp.where((seed_ref[pl.ds(8 * q, 8), :] > 0) | (vid == source), 1, 0)
        x = x << (lane % 32)
        for sh in (1, 2, 4, 8, 16):
            x = x | pltpu.roll(x, 128 - sh, 1)
        x = gather_lanes(x, 32 * (word_of % 4))
        words = words | jnp.where(word_of // 4 == sub + 8 * q, x, 0)
    for sh in (4, 2, 1):
        words = words | pltpu.roll(words, sh, 0)

    def spread_col(words):
        def step(k, acc_all):
            acc = zero
            for b in range(32):
                bit = (1 << b) if b < 31 else -(1 << 31)
                acc = acc | jnp.where((words_ref[k * 32 + b] & words) != 0, bit, 0)
            sh = 1
            while sh < wd:
                acc = acc | pltpu.roll(acc, 128 - sh, 1)
                sh *= 2
            got = gather_lanes(acc, wd * ((lane % K) // KG))
            return acc_all | jnp.where(lane % KG == k, got, 0)

        nxt = repeat(KG, step, zero)
        at = me_r * (height // 32) + sub * K + lane % K - me_c * wd
        now = gather_lanes(words, jnp.clip(at, 0, wd - 1))
        now = jnp.where((at >= 0) & (at < wd), now, 0)
        nxt = nxt | now
        tiles = []
        for t in range(NTC):
            sh = t * NB + lane // K
            tiles.append((lax.shift_right_logical(nxt, sh) & PAIR)
                         | ((lax.shift_right_logical(now, sh) & PAIR) << 1))
        return tiles

    def exchange(axis, count, me, slot, send, recv):
        copies = []
        order = sorted(range(1, count), key=lambda s: -min(s, count - s))
        for step in order:
            copy = pltpu.make_async_remote_copy(
                src_ref=slot.at[0], dst_ref=slot.at[step],
                send_sem=send.at[step], recv_sem=recv.at[step],
                device_id={axis: lax.rem(me + step, count)}, device_id_type=MESH)
            copy.start()
            copies.append(copy)
        return copies

    def join_col(slot, copies):
        for copy in copies:
            copy.wait_recv()
        nxt = zero
        now = zero
        for t in range(NTC):
            code = slot[0, t]
            for step in range(1, C):
                code = code | slot[step, t]
            sh = t * NB + lane // K
            nxt = nxt | ((code & PAIR) << sh)
            now = now | ((lax.shift_right_logical(code, 1) & PAIR) << sh)
        sh = K
        while sh < 128:
            nxt = nxt | pltpu.roll(nxt, sh, 1)
            now = now | pltpu.roll(now, sh, 1)
            sh *= 2
        return nxt, now

    def row_words(rows, k):
        return gather_lanes(rows, (lane // wd) * KG + k)

    def all_or(x):
        sh = wd
        while sh < 128:
            x = x | pltpu.roll(x, sh, 1)
            sh *= 2
        for sh in (4, 2, 1):
            x = x | pltpu.roll(x, sh, 0)
        return x

    def push(rows):
        def step(k, out):
            f = row_words(rows, k)
            for b in range(32):
                out = out | (words_ref[k * 32 + b] & ((f << (31 - b)) >> 31))
            return out

        out = repeat(KG, step, zero)
        at = me_c * wd + word_of - me_r * (height // 32)
        ok = (at >= 0) & (at < height // 32)
        at = jnp.clip(at, 0, height // 32 - 1)
        own = gather_lanes(rows, at % K)
        return all_or(out | jnp.where(ok & (at // K == sub), own, 0))

    def tournament(rows):
        kbits = log2(KG)

        def step(k, carry):
            f = row_words(rows, k)
            nodes = [[words_ref[k * 32 + b] & ((f << (31 - b)) >> 31)] for b in range(32)]
            while len(nodes) > 1:
                nodes = [merge(nodes[i], nodes[i + 1]) for i in range(0, len(nodes), 2)]
            node = nodes[0]
            fresh = node[0] & ~carry[0]
            rest = ~carry[0]
            out = [carry[0] | node[0]]
            for p in range(5):
                out.append(carry[1 + p] | (node[1 + p] & rest))
            for p in range(kbits):
                out.append(carry[6 + p] | (fresh & -((k >> p) & 1)))
            return tuple(out)

        return list(repeat(KG, step, (zero,) * (6 + kbits)))

    slot_bit = sub * G + lane // wd

    for t, tile in enumerate(spread_col(words)):
        col_buf[0, 0, t] = tile
    pl.semaphore_wait(barrier, R + C - 2)
    pend1 = exchange("col", C, me_c, col_buf.at[0], col_send.at[0], col_recv.at[0])
    s1, s0 = join_col(col_buf.at[0], pend1)

    out = push(s1)
    for t in range(NTR):
        row_buf[0, t] = lax.shift_right_logical(out, slot_bit + t * 8 * G) & 1
    pend2 = exchange("row", R, me_r, row_buf, row_send, row_recv)
    first_two = [tournament(s0), tournament(s1)]
    for copy in pend2:
        copy.wait_recv()
    words = zero
    for t in range(NTR):
        value = row_buf[0, t]
        for step in range(1, R):
            value = value | row_buf[step, t]
        words = words | (value << (slot_bit + t * 8 * G))
    words = all_or(words)

    for t, tile in enumerate(spread_col(words)):
        col_buf[1, 0, t] = tile
    pend3 = exchange("col", C, me_c, col_buf.at[1], col_send.at[1], col_recv.at[1])
    s3, s2 = join_col(col_buf.at[1], pend3)

    nodes = first_two + [tournament(s2), tournament(s3)]
    have = [node[0] for node in nodes]
    planes = list(nodes[0][1:])
    for d in range(1, LEVELS):
        fresh = have[d] & ~have[d - 1]
        planes = [p | (q & fresh) for p, q in zip(planes, nodes[d][1:])]

    def fold(have, planes, sh, axis, size):
        have_hi = [pltpu.roll(x, size - sh, axis) for x in have]
        planes_hi = [pltpu.roll(x, size - sh, axis) for x in planes]
        better = have_hi[0] & ~have[0]
        for a, b in zip(have[1:], have_hi[1:]):
            better = better | (b & ~a)
        keep = ~better
        planes = [(a & keep) | (b & better) for a, b in zip(planes, planes_hi)] + [better]
        return [a | b for a, b in zip(have, have_hi)], planes

    for i in range(log2(G)):
        have, planes = fold(have, planes, wd << i, 1, 128)
    for i in range(3):
        have, planes = fold(have, planes, 1 << i, 0, 8)

    have = [jnp.broadcast_to(x[0:1, :], (8, 128)) for x in have]
    planes = [jnp.broadcast_to(x[0:1, :], (8, 128)) for x in planes]
    for q in range(seed_ref.shape[0] // 8):
        idx = (sub + 8 * q) * 4 + lane // 32

        def bits(x):
            return lax.shift_right_logical(gather_lanes(x, idx), lane % 32) & 1

        key = jnp.full((8, 128), LEVELS * total, jnp.int32)
        for x in have:
            key = key - bits(x) * total
        parent = jnp.full((8, 128), me_r * height, jnp.int32)
        for p, x in enumerate(planes):
            parent = parent + (bits(x) << p)
        key_buf[0, q] = key + parent
    pend4 = exchange("row", R, me_r, key_buf, key_send, key_recv)
    for copy in pend4:
        copy.wait_recv()
    for q in range(seed_ref.shape[0] // 8):
        key = key_buf[0, q]
        for step in range(1, R):
            key = jnp.minimum(key, key_buf[step, q])
        level = jnp.full((8, 128), 1, jnp.int32)
        parent = key
        for d in range(1, LEVELS):
            past = key >= d * total
            level = level + jnp.where(past, 1, 0)
            parent = parent - jnp.where(past, total, 0)
        none = key >= LEVELS * total
        level = jnp.where(none, -1, level)
        parent = jnp.where(none, -1, parent)
        vid = first + (sub + 8 * q) * 128 + lane
        seed = (seed_ref[pl.ds(8 * q, 8), :] > 0) | (vid == source)
        lev_ref[pl.ds(8 * q, 8), :] = jnp.where(seed, 0, level)
        par_ref[pl.ds(8 * q, 8), :] = jnp.where(seed, vid, parent)
    for copy in pend1 + pend2 + pend3 + pend4:
        copy.wait_send()


def solution(mesh):
    R, C = mesh.shape["row"], mesh.shape["col"]

    def local(adjacency, seed_mask, source):
        height, wd = adjacency.shape
        width = seed_mask.shape[0]
        K = height // 256
        G = 128 // wd
        NTC = 16 // (128 // K)
        NTR = 4 // G
        NK = width // 1024
        out = jax.ShapeDtypeStruct((width // 128, 128), jnp.int32)
        vmem = pl.BlockSpec(memory_space=pltpu.VMEM)
        DMA = pltpu.SemaphoreType.DMA
        levels, parents = pl.pallas_call(
            functools.partial(kernel, R, C),
            out_shape=(out, out),
            in_specs=[vmem, vmem, pl.BlockSpec(memory_space=pltpu.SMEM)],
            out_specs=(vmem, vmem),
            scratch_shapes=[
                pltpu.VMEM((height // 8 // G, 8, 128), jnp.int32),
                pltpu.VMEM((2, C, NTC, 8, 128), jnp.int32),
                pltpu.VMEM((R, NTR, 8, 128), jnp.int32),
                pltpu.VMEM((R, NK, 8, 128), jnp.int32),
                DMA((2, C)), DMA((2, C)), DMA((R,)), DMA((R,)), DMA((R,)), DMA((R,)),
            ],
            compiler_params=pltpu.CompilerParams(collective_id=0, has_side_effects=True),
        )(adjacency, seed_mask.reshape(width // 128, 128), source)
        return levels.reshape(width), parents.reshape(width)

    in_specs = (P("row", "col"), P("col"), P())
    out_specs = (P("col"), P("col"))
    return jax.shard_map(local, mesh=mesh, in_specs=in_specs, out_specs=out_specs, check_vma=False)
```

```python
import functools

import jax
import jax.numpy as jnp
from jax import lax
from jax.experimental import pallas as pl
from jax.experimental.pallas import tpu as pltpu
from jax.sharding import PartitionSpec as P

LEVELS = 4
MESH = pl.DeviceIdType.MESH
PAIR = 0x10001


def log2(n):
    return n.bit_length() - 1


def gather_lanes(x, idx):
    return jnp.take_along_axis(x, idx, axis=1)


def any_of(values):
    values = list(values)
    while len(values) > 1:
        pairs = [values[i] | values[i + 1] for i in range(0, len(values) - 1, 2)]
        values = pairs + values[len(pairs) * 2:]
    return values[0]


def repeat(n, body, init):
    if n <= 4:
        for i in range(n):
            init = body(i, init)
        return init
    return lax.fori_loop(0, n, body, init)


def merge(low, high):
    rest = ~low[0]
    out = [low[0] | high[0]]
    for a, b in zip(low[1:], high[1:]):
        out.append(a | (b & rest))
    out.append(high[0] & rest)
    return out


def kernel(R, C, hbm_ref, seed_ref, src_ref, key_ref,
           adj_ref, load_sem, turn_ref, words_ref, col_buf, row_buf, key_buf,
           col_send, col_recv, row_send, row_recv, key_send, key_recv):
    me_r = lax.axis_index("row")
    me_c = lax.axis_index("col")
    wd, height = hbm_ref.shape
    loads = [pltpu.make_async_copy(hbm_ref.at[:, pl.ds(128 * t, 128)], adj_ref.at[pl.ds(wd * t, wd), :], load_sem.at[t])
             for t in range(height // 128)]
    for load in loads:
        load.start()
    G = 128 // wd
    NI = wd // 32
    NR = height // 1024
    NK = height // 128 // G
    owners = NR // NI
    total = R * height

    barrier = pltpu.get_barrier_semaphore()
    for step in range(1, C):
        pl.semaphore_signal(barrier, inc=1, device_id={"col": lax.rem(me_c + step, C)}, device_id_type=MESH)
    for step in range(1, R):
        pl.semaphore_signal(barrier, inc=1, device_id={"row": lax.rem(me_r + step, R)}, device_id_type=MESH)

    lane = lax.broadcasted_iota(jnp.int32, (8, 128), 1)
    sub = lax.broadcasted_iota(jnp.int32, (8, 128), 0)
    bit = lane % 32
    zero = jnp.zeros((8, 128), jnp.int32)
    source = src_ref[0]
    first = me_c * (wd * 32)

    def seeds(q):
        vid = first + (sub + 8 * q) * 128 + lane
        return (seed_ref[pl.ds(8 * q, 8), :] > 0) | (vid == source), vid

    def block(a, q, t):
        return adj_ref[pl.ds(wd * t + 32 * a + q, 8, stride=4), :]

    def pull(col_set):
        words = []
        for tile in col_set:
            x = tile << bit
            for sh in (1, 2, 4, 8, 16):
                x = x | pltpu.roll(x, 128 - sh, 1)
            words.append([gather_lanes(x, zero + 32 * q) for q in range(4)])
        codes = []
        for h in range(NR):
            accs = [any_of(block(a, q, 8 * h + t) & words[a][q] for a in range(NI) for q in range(4))
                    for t in range(8)]
            for sh in (4, 2, 1):
                low = (sub // sh) % 2 == 0
                half = []
                for t in range(sh):
                    keep = jnp.where(low, accs[t], accs[t + sh])
                    give = jnp.where(low, accs[t + sh], accs[t])
                    if sh == 4:
                        other = pltpu.roll(give, 4, 0)
                    else:
                        other = jnp.where(low, pltpu.roll(give, 8 - sh, 0), pltpu.roll(give, sh, 0))
                    half.append(keep | other)
                accs = half
            code = jnp.where(accs[0] != 0, 1, 0)
            own = me_c == me_r * owners + h // NI
            codes.append(code | jnp.where(own, 3 * col_set[h % NI], 0))
        return [codes[h] | (codes[h + NR // 2] << 16) for h in range(NR // 2)]

    def push(row_set):
        out = [[zero] * 4 for _ in range(NI)]
        for t in range(8 * NR):
            mask = jnp.broadcast_to(row_set[t // 8][t % 8:t % 8 + 1, :], (8, 128))
            for a in range(NI):
                for q in range(4):
                    out[a][q] = out[a][q] | (block(a, q, t) & mask)
        result = []
        for a in range(NI):
            parts = out[a]
            for sh in (64, 32):
                low = (lane // sh) % 2 == 0
                half = []
                for q in range(sh // 32):
                    keep = jnp.where(low, parts[q], parts[q + sh // 32])
                    give = jnp.where(low, parts[q + sh // 32], parts[q])
                    half.append(keep | gather_lanes(give, lane ^ sh))
                parts = half
            x = parts[0]
            for sh in (1, 2, 4, 8, 16):
                x = x | gather_lanes(x, lane ^ sh)
            value = lax.shift_right_logical(x, bit) & 1
            for o in range(owners):
                own = me_c == me_r * owners + o
                value = value | jnp.where(own, row_set[o * NI + a] & 1, 0)
            result.append(value)
        return result

    def exchange(axis, count, me, slot, send, recv):
        copies = []
        order = sorted(range(1, count), key=lambda s: -min(s, count - s))
        for step in order:
            copy = pltpu.make_async_remote_copy(
                src_ref=slot.at[0], dst_ref=slot.at[step],
                send_sem=send.at[step], recv_sem=recv.at[step],
                device_id={axis: lax.rem(me + step, count)}, device_id_type=MESH)
            copy.start()
            copies.append(copy)
        return copies

    def join_col(slot, copies):
        for copy in copies:
            copy.wait_recv()
        pairs = [any_of(slot[step, t] for step in range(C)) for t in range(NR // 2)]
        codes = pairs + [x >> 16 for x in pairs]
        return [(x << 31) >> 31 for x in codes], [(x << 30) >> 31 for x in codes]

    def turn():
        def step(k, carry):
            parts = [adj_ref[pl.ds(pl.multiple_of((NK * g + k) * wd, 8), wd), :] for g in range(G)]
            x = parts[0] if G == 1 else jnp.concatenate(parts, axis=0)
            turn_ref[...] = x.T
            for j in range(16):
                words_ref[k * 16 + j] = turn_ref[pl.ds(j, 8, stride=16), :]
            return carry

        repeat(NK, step, 0)

    def row_words(row_set):
        for h, mask in enumerate(row_set):
            x = (mask & 1) << (lane % 16)
            for sh in (1, 2, 4, 8):
                x = x | pltpu.roll(x, 128 - sh, 1)
            turn_ref[pl.ds(8 * h, 8), :] = x

    def tournament(row_set):
        kbits = log2(NK)
        row_words(row_set)

        def step(k, carry):
            f = zero
            for g in range(G):
                row = jnp.broadcast_to(turn_ref[pl.ds(NK * g + k, 1), :], (8, 128))
                f = jnp.where(lane // wd == g, gather_lanes(row, sub * 16), f)
            nodes = [[words_ref[k * 16 + j] & ((f << (31 - j)) >> 31)] for j in range(16)]
            while len(nodes) > 1:
                nodes = [merge(nodes[i], nodes[i + 1]) for i in range(0, len(nodes), 2)]
            node = nodes[0]
            rest = ~carry[0]
            fresh = node[0] & rest
            out = [carry[0] | node[0]]
            for p in range(4):
                out.append(carry[1 + p] | (node[1 + p] & rest))
            for p in range(kbits):
                out.append(carry[5 + p] | (fresh & -((k >> p) & 1)))
            return tuple(out)

        return list(repeat(NK, step, (zero,) * (5 + kbits)))

    for load in loads:
        load.wait()
    for t, tile in enumerate(pull([jnp.where(seeds(q)[0], 1, 0) for q in range(NI)])):
        col_buf[0, 0, t] = tile
    pl.semaphore_wait(barrier, R + C - 2)
    pend1 = exchange("col", C, me_c, col_buf.at[0], col_send.at[0], col_recv.at[0])
    turn()
    s1, s0 = join_col(col_buf.at[0], pend1)

    for t, tile in enumerate(push(s1)):
        row_buf[0, t] = tile
    pend2 = exchange("row", R, me_r, row_buf, row_send, row_recv)
    first_two = [tournament(s0), tournament(s1)]
    for copy in pend2:
        copy.wait_recv()
    col_set = [any_of(row_buf[step, t] for step in range(R)) for t in range(NI)]

    for t, tile in enumerate(pull(col_set)):
        col_buf[1, 0, t] = tile
    pend3 = exchange("col", C, me_c, col_buf.at[1], col_send.at[1], col_recv.at[1])
    s3, s2 = join_col(col_buf.at[1], pend3)

    nodes = first_two + [tournament(s2), tournament(s3)]
    have = [node[0] for node in nodes]
    planes = list(nodes[0][1:])
    for d in range(1, LEVELS):
        fresh = have[d] & ~have[d - 1]
        planes = [p | (q & fresh) for p, q in zip(planes, nodes[d][1:])]
    kbits = log2(NK)
    where = list(range(4)) + [7 + p for p in range(kbits)]

    def fold(have, planes, turned, by_step):
        have_hi = [turned(x) for x in have]
        planes_hi = [turned(x) for x in planes]
        better = any_of(b & ~a for a, b in zip(have, have_hi))
        if by_step:
            same = ~any_of(a ^ b for a, b in zip(have, have_hi))
            less = None
            for a, b in zip(planes[4:4 + kbits], planes_hi[4:4 + kbits]):
                now = a & ~b
                less = now if less is None else now | (less & ~(a ^ b))
            if less is not None:
                better = better | (same & less)
        keep = ~better
        planes = [(a & keep) | (b & better) for a, b in zip(planes, planes_hi)] + [better]
        return [a | b for a, b in zip(have, have_hi)], planes

    for i in range(3):
        have, planes = fold(have, planes, lambda x: pltpu.roll(x, 8 - (1 << i), 0), True)
        where.append(4 + i)
    for i in range(log2(G)):
        have, planes = fold(have, planes, lambda x: pltpu.roll(x, 128 - (wd << i), 1), False)
        where.append(7 + kbits + i)

    have = [jnp.broadcast_to(x[0:1, :], (8, 128)) for x in have]
    planes = [jnp.broadcast_to(x[0:1, :], (8, 128)) for x in planes]
    for q in range(NI):
        idx = (sub + 8 * q) * 4 + lane // 32

        def bits(x):
            return lax.shift_right_logical(gather_lanes(x, idx), bit) & 1

        key = jnp.full((8, 128), (LEVELS + 1) * total, jnp.int32)
        for x in have:
            key = key - bits(x) * total
        parent = jnp.full((8, 128), me_r * height, jnp.int32)
        for p, x in zip(where, planes):
            parent = parent + (bits(x) << p)
        key_buf[0, q] = key + parent
    pend4 = exchange("row", R, me_r, key_buf, key_send, key_recv)
    for copy in pend4:
        copy.wait_recv()
    for q in range(NI):
        key = key_buf[0, q]
        for step in range(1, R):
            key = jnp.minimum(key, key_buf[step, q])
        seed, vid = seeds(q)
        key_ref[pl.ds(8 * q, 8), :] = jnp.where(seed, vid, key)
    for copy in pend1 + pend2 + pend3 + pend4:
        copy.wait_send()


def solution(mesh):
    R, C = mesh.shape["row"], mesh.shape["col"]

    def local(adjacency, seed_mask, source):
        height, wd = adjacency.shape
        width = seed_mask.shape[0]
        total = R * height
        G = 128 // wd
        NI = width // 1024
        NR = height // 1024
        vmem = pl.BlockSpec(memory_space=pltpu.VMEM)
        DMA = pltpu.SemaphoreType.DMA
        key = pl.pallas_call(
            functools.partial(kernel, R, C),
            out_shape=jax.ShapeDtypeStruct((width // 128, 128), jnp.int32),
            in_specs=[pl.BlockSpec(memory_space=pl.ANY), vmem, pl.BlockSpec(memory_space=pltpu.SMEM)],
            out_specs=vmem,
            scratch_shapes=[
                pltpu.VMEM((height // 128 * wd, 128), jnp.int32),
                DMA((height // 128,)),
                pltpu.VMEM((128, 128), jnp.int32),
                pltpu.VMEM((height // 8 // G, 8, 128), jnp.int32),
                pltpu.VMEM((2, C, NR // 2, 8, 128), jnp.int32),
                pltpu.VMEM((R, NI, 8, 128), jnp.int32),
                pltpu.VMEM((R, NI, 8, 128), jnp.int32),
                DMA((2, C)), DMA((2, C)), DMA((R,)), DMA((R,)), DMA((R,)), DMA((R,)),
            ],
            compiler_params=pltpu.CompilerParams(collective_id=0, has_side_effects=True),
        )(adjacency.T, seed_mask.reshape(width // 128, 128), source)
        key = key.reshape(width)
        level = jnp.zeros_like(key)
        for d in range(1, LEVELS + 1):
            level = level + (key >= d * total).astype(jnp.int32)
        none = key >= (LEVELS + 1) * total
        return jnp.where(none, -1, level), jnp.where(none, -1, key - level * total)

    in_specs = (P("row", "col"), P("col"), P())
    out_specs = (P("col"), P("col"))
    return jax.shard_map(local, mesh=mesh, in_specs=in_specs, out_specs=out_specs, check_vma=False)
```

```python
import functools

import jax
import jax.numpy as jnp
from jax import lax
from jax.experimental import pallas as pl
from jax.experimental.pallas import tpu as pltpu
from jax.sharding import PartitionSpec as P

LEVELS = 4
MESH = pl.DeviceIdType.MESH
PAIR = 0x10001


def log2(n):
    return n.bit_length() - 1


def gather_lanes(x, idx):
    return jnp.take_along_axis(x, idx, axis=1)


def far_first(count):
    return sorted(range(1, count), key=lambda s: -min(s, count - s))


def any_of(values):
    values = list(values)
    while len(values) > 1:
        pairs = [values[i] | values[i + 1] for i in range(0, len(values) - 1, 2)]
        values = pairs + values[len(pairs) * 2:]
    return values[0]


def repeat(n, body, init):
    if n <= 4:
        for i in range(n):
            init = body(i, init)
        return init
    return lax.fori_loop(0, n, body, init)


def merge(low, high):
    rest = ~low[0]
    out = [low[0] | high[0]]
    for a, b in zip(low[1:], high[1:]):
        out.append(a | (b & rest))
    out.append(high[0] & rest)
    return out


def kernel(R, C, hbm_ref, seed_hbm, src_ref, key_ref,
           adj_ref, load_sem, seed_ref, small_sem, turn_ref, words_ref, col_buf, row_buf, key_buf,
           col_send, col_recv, row_send, row_recv, key_send, key_recv):
    me_r = lax.axis_index("row")
    me_c = lax.axis_index("col")
    barrier = pltpu.get_barrier_semaphore()
    for step in far_first(C):
        pl.semaphore_signal(barrier, inc=1, device_id={"col": lax.rem(me_c + step, C)}, device_id_type=MESH)
    for step in far_first(R):
        pl.semaphore_signal(barrier, inc=1, device_id={"row": lax.rem(me_r + step, R)}, device_id_type=MESH)

    wd, height = hbm_ref.shape
    small = pltpu.make_async_copy(seed_hbm, seed_ref, small_sem)
    loads = [pltpu.make_async_copy(hbm_ref.at[:, pl.ds(128 * t, 128)], adj_ref.at[pl.ds(wd * t, wd), :], load_sem.at[t])
             for t in range(height // 128)]
    for load in [small] + loads:
        load.start()
    G = 128 // wd
    NI = wd // 32
    NR = height // 1024
    NK = height // 128 // G
    owners = NR // NI
    total = R * height

    lane = lax.broadcasted_iota(jnp.int32, (8, 128), 1)
    sub = lax.broadcasted_iota(jnp.int32, (8, 128), 0)
    bit = lane % 32
    zero = jnp.zeros((8, 128), jnp.int32)
    small.wait()
    source = src_ref[0]
    first = me_c * (wd * 32)

    def seeds(q):
        vid = first + (sub + 8 * q) * 128 + lane
        return (seed_ref[pl.ds(8 * q, 8), :] > 0) | (vid == source), vid

    def block(a, q, t):
        return adj_ref[pl.ds(wd * t + 32 * a + q, 8, stride=4), :]

    def pull(col_set):
        words = []
        for tile in col_set:
            x = tile << bit
            for sh in (1, 2, 4, 8, 16):
                x = x | pltpu.roll(x, 128 - sh, 1)
            words.append([gather_lanes(x, zero + 32 * q) for q in range(4)])
        codes = []
        for h in range(NR):
            accs = [any_of(block(a, q, 8 * h + t) & words[a][q] for a in range(NI) for q in range(4))
                    for t in range(8)]
            for sh in (4, 2, 1):
                low = (sub // sh) % 2 == 0
                half = []
                for t in range(sh):
                    keep = jnp.where(low, accs[t], accs[t + sh])
                    give = jnp.where(low, accs[t + sh], accs[t])
                    if sh == 4:
                        other = pltpu.roll(give, 4, 0)
                    else:
                        other = jnp.where(low, pltpu.roll(give, 8 - sh, 0), pltpu.roll(give, sh, 0))
                    half.append(keep | other)
                accs = half
            code = jnp.where(accs[0] != 0, 1, 0)
            own = me_c == me_r * owners + h // NI
            codes.append(code | jnp.where(own, 3 * col_set[h % NI], 0))
        return [codes[h] | (codes[h + NR // 2] << 16) for h in range(NR // 2)]

    def push(row_set):
        out = [[zero] * 4 for _ in range(NI)]
        for t in range(8 * NR):
            mask = jnp.broadcast_to(row_set[t // 8][t % 8:t % 8 + 1, :], (8, 128))
            for a in range(NI):
                for q in range(4):
                    out[a][q] = out[a][q] | (block(a, q, t) & mask)
        result = []
        for a in range(NI):
            parts = out[a]
            for sh in (64, 32):
                low = (lane // sh) % 2 == 0
                half = []
                for q in range(sh // 32):
                    keep = jnp.where(low, parts[q], parts[q + sh // 32])
                    give = jnp.where(low, parts[q + sh // 32], parts[q])
                    half.append(keep | gather_lanes(give, lane ^ sh))
                parts = half
            x = parts[0]
            for sh in (1, 2, 4, 8, 16):
                x = x | gather_lanes(x, lane ^ sh)
            value = lax.shift_right_logical(x, bit) & 1
            for o in range(owners):
                own = me_c == me_r * owners + o
                value = value | jnp.where(own, row_set[o * NI + a] & 1, 0)
            result.append(value)
        return result

    def exchange(axis, count, me, slot, send, recv):
        copies = []
        for step in far_first(count):
            copy = pltpu.make_async_remote_copy(
                src_ref=slot.at[0], dst_ref=slot.at[step],
                send_sem=send.at[step], recv_sem=recv.at[step],
                device_id={axis: lax.rem(me + step, count)}, device_id_type=MESH)
            copy.start()
            copies.append(copy)
        return copies

    def join_col(slot, copies):
        for copy in copies:
            copy.wait_recv()
        pairs = [any_of(slot[step, t] for step in range(C)) for t in range(NR // 2)]
        codes = pairs + [x >> 16 for x in pairs]
        return [(x << 31) >> 31 for x in codes], [(x << 30) >> 31 for x in codes]

    def turn():
        def step(k, carry):
            parts = [adj_ref[pl.ds(pl.multiple_of((NK * g + k) * wd, 8), wd), :] for g in range(G)]
            x = parts[0] if G == 1 else jnp.concatenate(parts, axis=0)
            turn_ref[...] = x.T
            for j in range(16):
                words_ref[k * 16 + j] = turn_ref[pl.ds(j, 8, stride=16), :]
            return carry

        repeat(NK, step, 0)

    def row_words(row_set):
        for h, mask in enumerate(row_set):
            x = (mask & 1) << (lane % 16)
            for sh in (1, 2, 4, 8):
                x = x | pltpu.roll(x, 128 - sh, 1)
            turn_ref[pl.ds(8 * h, 8), :] = x

    def tournament(row_set):
        kbits = log2(NK)
        row_words(row_set)

        def step(k, carry):
            f = zero
            for g in range(G):
                row = jnp.broadcast_to(turn_ref[pl.ds(NK * g + k, 1), :], (8, 128))
                f = jnp.where(lane // wd == g, gather_lanes(row, sub * 16), f)
            nodes = [[words_ref[k * 16 + j] & ((f << (31 - j)) >> 31)] for j in range(16)]
            while len(nodes) > 1:
                nodes = [merge(nodes[i], nodes[i + 1]) for i in range(0, len(nodes), 2)]
            node = nodes[0]
            rest = ~carry[0]
            fresh = node[0] & rest
            out = [carry[0] | node[0]]
            for p in range(4):
                out.append(carry[1 + p] | (node[1 + p] & rest))
            for p in range(kbits):
                out.append(carry[5 + p] | (fresh & -((k >> p) & 1)))
            return tuple(out)

        return list(repeat(NK, step, (zero,) * (5 + kbits)))

    for load in loads:
        load.wait()
    for t, tile in enumerate(pull([jnp.where(seeds(q)[0], 1, 0) for q in range(NI)])):
        col_buf[0, 0, t] = tile
    pl.semaphore_wait(barrier, R + C - 2)
    pend1 = exchange("col", C, me_c, col_buf.at[0], col_send.at[0], col_recv.at[0])
    turn()
    s1, s0 = join_col(col_buf.at[0], pend1)

    for t, tile in enumerate(push(s1)):
        row_buf[0, t] = tile
    pend2 = exchange("row", R, me_r, row_buf, row_send, row_recv)
    first_two = [tournament(s0), tournament(s1)]
    for copy in pend2:
        copy.wait_recv()
    col_set = [any_of(row_buf[step, t] for step in range(R)) for t in range(NI)]

    for t, tile in enumerate(pull(col_set)):
        col_buf[1, 0, t] = tile
    pend3 = exchange("col", C, me_c, col_buf.at[1], col_send.at[1], col_recv.at[1])
    s3, s2 = join_col(col_buf.at[1], pend3)

    nodes = first_two + [tournament(s2), tournament(s3)]
    have = [node[0] for node in nodes]
    planes = list(nodes[0][1:])
    for d in range(1, LEVELS):
        fresh = have[d] & ~have[d - 1]
        planes = [p | (q & fresh) for p, q in zip(planes, nodes[d][1:])]
    kbits = log2(NK)
    where = list(range(4)) + [7 + p for p in range(kbits)]

    def fold(have, planes, turned, by_step):
        have_hi = [turned(x) for x in have]
        planes_hi = [turned(x) for x in planes]
        better = any_of(b & ~a for a, b in zip(have, have_hi))
        if by_step:
            same = ~any_of(a ^ b for a, b in zip(have, have_hi))
            less = None
            for a, b in zip(planes[4:4 + kbits], planes_hi[4:4 + kbits]):
                now = a & ~b
                less = now if less is None else now | (less & ~(a ^ b))
            if less is not None:
                better = better | (same & less)
        keep = ~better
        planes = [(a & keep) | (b & better) for a, b in zip(planes, planes_hi)] + [better]
        return [a | b for a, b in zip(have, have_hi)], planes

    for i in range(3):
        have, planes = fold(have, planes, lambda x: pltpu.roll(x, 8 - (1 << i), 0), True)
        where.append(4 + i)
    for i in range(log2(G)):
        have, planes = fold(have, planes, lambda x: pltpu.roll(x, 128 - (wd << i), 1), False)
        where.append(7 + kbits + i)

    have = [jnp.broadcast_to(x[0:1, :], (8, 128)) for x in have]
    planes = [jnp.broadcast_to(x[0:1, :], (8, 128)) for x in planes]
    for q in range(NI):
        idx = (sub + 8 * q) * 4 + lane // 32

        def bits(x):
            return lax.shift_right_logical(gather_lanes(x, idx), bit) & 1

        key = jnp.full((8, 128), (LEVELS + 1) * total, jnp.int32)
        for x in have:
            key = key - bits(x) * total
        parent = jnp.full((8, 128), me_r * height, jnp.int32)
        for p, x in zip(where, planes):
            parent = parent + (bits(x) << p)
        key_buf[0, q] = key + parent
    pend4 = exchange("row", R, me_r, key_buf, key_send, key_recv)
    for copy in pend4:
        copy.wait_recv()
    for q in range(NI):
        key = key_buf[0, q]
        for step in range(1, R):
            key = jnp.minimum(key, key_buf[step, q])
        seed, vid = seeds(q)
        key_ref[pl.ds(8 * q, 8), :] = jnp.where(seed, vid, key)
    for copy in pend1 + pend2 + pend3 + pend4:
        copy.wait_send()


def solution(mesh):
    R, C = mesh.shape["row"], mesh.shape["col"]

    def local(adjacency, seed_mask, source):
        height, wd = adjacency.shape
        width = seed_mask.shape[0]
        total = R * height
        G = 128 // wd
        NI = width // 1024
        NR = height // 1024
        vmem = pl.BlockSpec(memory_space=pltpu.VMEM)
        DMA = pltpu.SemaphoreType.DMA
        key = pl.pallas_call(
            functools.partial(kernel, R, C),
            out_shape=pltpu.VMEM((width // 128, 128), jnp.int32),
            in_specs=[pl.BlockSpec(memory_space=pl.ANY)] * 2 + [pl.BlockSpec(memory_space=pltpu.SMEM)],
            out_specs=vmem,
            scratch_shapes=[
                pltpu.VMEM((height // 128 * wd, 128), jnp.int32),
                DMA((height // 128,)),
                pltpu.VMEM((width // 128, 128), jnp.int32),
                DMA(()),
                pltpu.VMEM((128, 128), jnp.int32),
                pltpu.VMEM((height // 8 // G, 8, 128), jnp.int32),
                pltpu.VMEM((2, C, NR // 2, 8, 128), jnp.int32),
                pltpu.VMEM((R, NI, 8, 128), jnp.int32),
                pltpu.VMEM((R, NI, 8, 128), jnp.int32),
                DMA((2, C)), DMA((2, C)), DMA((R,)), DMA((R,)), DMA((R,)), DMA((R,)),
            ],
            compiler_params=pltpu.CompilerParams(collective_id=0, has_side_effects=True),
        )(adjacency.T, seed_mask.reshape(width // 128, 128), source)
        key = key.reshape(width)
        level = jnp.zeros_like(key)
        for d in range(1, LEVELS + 1):
            level = level + (key >= d * total).astype(jnp.int32)
        none = key >= (LEVELS + 1) * total
        return jnp.where(none, -1, level), jnp.where(none, -1, key - level * total)

    in_specs = (P("row", "col"), P("col"), P())
    out_specs = (P("col"), P("col"))
    return jax.shard_map(local, mesh=mesh, in_specs=in_specs, out_specs=out_specs, check_vma=False)
```

```python
import functools

import jax
import jax.numpy as jnp
from jax import lax
from jax.experimental import pallas as pl
from jax.experimental.pallas import tpu as pltpu
from jax.sharding import PartitionSpec as P

LEVELS = 4
MESH = pl.DeviceIdType.MESH
PAIR = 0x10001


def log2(n):
    return n.bit_length() - 1


def gather_lanes(x, idx):
    return jnp.take_along_axis(x, idx, axis=1)


def far_first(count):
    return sorted(range(1, count), key=lambda s: -min(s, count - s))


def any_of(values):
    values = list(values)
    while len(values) > 1:
        pairs = [values[i] | values[i + 1] for i in range(0, len(values) - 1, 2)]
        values = pairs + values[len(pairs) * 2:]
    return values[0]


def repeat(n, body, init):
    if n <= 4:
        for i in range(n):
            init = body(i, init)
        return init
    return lax.fori_loop(0, n, body, init)


def merge(low, high):
    rest = ~low[0]
    out = [low[0] | high[0]]
    for a, b in zip(low[1:], high[1:]):
        out.append(a | (b & rest))
    out.append(high[0] & rest)
    return out


def kernel(R, C, hbm_ref, seed_hbm, src_ref, key_ref,
           adj_ref, load_sem, seed_ref, small_sem, turn_ref, words_ref, col_buf, row_buf, key_buf,
           col_send, col_recv, row_send, row_recv, key_send, key_recv):
    me_r = lax.axis_index("row")
    me_c = lax.axis_index("col")
    barrier = pltpu.get_barrier_semaphore()
    for step in far_first(C):
        pl.semaphore_signal(barrier, inc=1, device_id={"col": lax.rem(me_c + step, C)}, device_id_type=MESH)
    for step in far_first(R):
        pl.semaphore_signal(barrier, inc=1, device_id={"row": lax.rem(me_r + step, R)}, device_id_type=MESH)

    wd, height = hbm_ref.shape
    small = pltpu.make_async_copy(seed_hbm, seed_ref, small_sem)
    loads = [pltpu.make_async_copy(hbm_ref.at[:, pl.ds(128 * t, 128)], adj_ref.at[pl.ds(wd * t, wd), :], load_sem.at[t])
             for t in range(height // 128)]
    for load in [small] + loads:
        load.start()
    G = 128 // wd
    NI = wd // 32
    NR = height // 1024
    NK = height // 128 // G
    owners = NR // NI
    total = R * height

    lane = lax.broadcasted_iota(jnp.int32, (8, 128), 1)
    sub = lax.broadcasted_iota(jnp.int32, (8, 128), 0)
    bit = lane % 32
    zero = jnp.zeros((8, 128), jnp.int32)
    small.wait()
    source = src_ref[0]
    first = me_c * (wd * 32)

    def seeds(q):
        vid = first + (sub + 8 * q) * 128 + lane
        return (seed_ref[pl.ds(8 * q, 8), :] > 0) | (vid == source), vid

    def block(a, q, t):
        return adj_ref[pl.ds(wd * t + 32 * a + q, 8, stride=4), :]

    def pull(col_set):
        words = []
        for tile in col_set:
            x = tile << bit
            for sh in (1, 2, 4, 8, 16):
                x = x | pltpu.roll(x, 128 - sh, 1)
            words.append([gather_lanes(x, zero + 32 * q) for q in range(4)])
        codes = []
        for h in range(NR):
            accs = [any_of(block(a, q, 8 * h + t) & words[a][q] for a in range(NI) for q in range(4))
                    for t in range(8)]
            for sh in (4, 2, 1):
                low = (sub // sh) % 2 == 0
                half = []
                for t in range(sh):
                    keep = jnp.where(low, accs[t], accs[t + sh])
                    give = jnp.where(low, accs[t + sh], accs[t])
                    if sh == 4:
                        other = pltpu.roll(give, 4, 0)
                    else:
                        other = jnp.where(low, pltpu.roll(give, 8 - sh, 0), pltpu.roll(give, sh, 0))
                    half.append(keep | other)
                accs = half
            code = jnp.where(accs[0] != 0, 1, 0)
            own = me_c == me_r * owners + h // NI
            codes.append(code | jnp.where(own, 3 * col_set[h % NI], 0))
        return [codes[h] | (codes[h + NR // 2] << 16) for h in range(NR // 2)]

    def push(row_set):
        out = [[zero] * 4 for _ in range(NI)]
        for t in range(8 * NR):
            mask = jnp.broadcast_to(row_set[t // 8][t % 8:t % 8 + 1, :], (8, 128))
            for a in range(NI):
                for q in range(4):
                    out[a][q] = out[a][q] | (block(a, q, t) & mask)
        result = []
        for a in range(NI):
            parts = out[a]
            for sh in (64, 32):
                low = (lane // sh) % 2 == 0
                half = []
                for q in range(sh // 32):
                    keep = jnp.where(low, parts[q], parts[q + sh // 32])
                    give = jnp.where(low, parts[q + sh // 32], parts[q])
                    half.append(keep | gather_lanes(give, lane ^ sh))
                parts = half
            x = parts[0]
            for sh in (1, 2, 4, 8, 16):
                x = x | gather_lanes(x, lane ^ sh)
            value = lax.shift_right_logical(x, bit) & 1
            for o in range(owners):
                own = me_c == me_r * owners + o
                value = value | jnp.where(own, row_set[o * NI + a] & 1, 0)
            result.append(value)
        return result

    def exchange(axis, count, me, slot, send, recv):
        copies = []
        for step in far_first(count):
            copy = pltpu.make_async_remote_copy(
                src_ref=slot.at[0], dst_ref=slot.at[step],
                send_sem=send.at[step], recv_sem=recv.at[step],
                device_id={axis: lax.rem(me + step, count)}, device_id_type=MESH)
            copy.start()
            copies.append(copy)
        return copies

    def join_col(slot, copies):
        for copy in copies:
            copy.wait_recv()
        pairs = [any_of(slot[step, t] for step in range(C)) for t in range(NR // 2)]
        codes = pairs + [x >> 16 for x in pairs]
        return [(x << 31) >> 31 for x in codes], [(x << 30) >> 31 for x in codes]

    def turn():
        def step(k, carry):
            parts = [adj_ref[pl.ds(pl.multiple_of((NK * g + k) * wd, 8), wd), :] for g in range(G)]
            x = parts[0] if G == 1 else jnp.concatenate(parts, axis=0)
            turn_ref[...] = x.T
            for j in range(16):
                words_ref[k * 16 + j] = turn_ref[pl.ds(j, 8, stride=16), :]
            return carry

        repeat(NK, step, 0)

    def row_words(nxt, now):
        at = lane % 16
        for h in range(NR):
            x = ((nxt[h] & 1) << at) | ((now[h] & 1) << (at + 16))
            for sh in (1, 2, 4, 8):
                x = x | pltpu.roll(x, 128 - sh, 1)
            turn_ref[pl.ds(8 * h, 8), :] = x

    def tournaments(nxt, now):
        kbits = log2(NK)
        row_words(nxt, now)

        def step(k, carries):
            f = zero
            for g in range(G):
                row = jnp.broadcast_to(turn_ref[pl.ds(NK * g + k, 1), :], (8, 128))
                f = jnp.where(lane // wd == g, gather_lanes(row, sub * 16), f)
            leaves = [words_ref[k * 16 + j] for j in range(16)]
            outs = []
            for top, carry in zip((15, 31), carries):
                nodes = [[leaves[j] & ((f << (top - j)) >> 31)] for j in range(16)]
                while len(nodes) > 1:
                    nodes = [merge(nodes[i], nodes[i + 1]) for i in range(0, len(nodes), 2)]
                node = nodes[0]
                rest = ~carry[0]
                fresh = node[0] & rest
                out = [carry[0] | node[0]]
                for p in range(4):
                    out.append(carry[1 + p] | (node[1 + p] & rest))
                for p in range(kbits):
                    out.append(carry[5 + p] | (fresh & -((k >> p) & 1)))
                outs.append(tuple(out))
            return tuple(outs)

        return list(repeat(NK, step, ((zero,) * (5 + kbits),) * 2))

    for load in loads:
        load.wait()
    for t, tile in enumerate(pull([jnp.where(seeds(q)[0], 1, 0) for q in range(NI)])):
        col_buf[0, 0, t] = tile
    pl.semaphore_wait(barrier, R + C - 2)
    pend1 = exchange("col", C, me_c, col_buf.at[0], col_send.at[0], col_recv.at[0])
    turn()
    s1, s0 = join_col(col_buf.at[0], pend1)

    for t, tile in enumerate(push(s1)):
        row_buf[0, t] = tile
    pend2 = exchange("row", R, me_r, row_buf, row_send, row_recv)
    first_two = tournaments(s1, s0)
    for copy in pend2:
        copy.wait_recv()
    col_set = [any_of(row_buf[step, t] for step in range(R)) for t in range(NI)]

    for t, tile in enumerate(pull(col_set)):
        col_buf[1, 0, t] = tile
    pend3 = exchange("col", C, me_c, col_buf.at[1], col_send.at[1], col_recv.at[1])
    s3, s2 = join_col(col_buf.at[1], pend3)

    nodes = first_two + tournaments(s3, s2)
    have = [node[0] for node in nodes]
    planes = list(nodes[0][1:])
    for d in range(1, LEVELS):
        fresh = have[d] & ~have[d - 1]
        planes = [p | (q & fresh) for p, q in zip(planes, nodes[d][1:])]
    kbits = log2(NK)
    where = list(range(4)) + [7 + p for p in range(kbits)]

    def fold(have, planes, turned, by_step):
        have_hi = [turned(x) for x in have]
        planes_hi = [turned(x) for x in planes]
        better = any_of(b & ~a for a, b in zip(have, have_hi))
        if by_step:
            same = ~any_of(a ^ b for a, b in zip(have, have_hi))
            less = None
            for a, b in zip(planes[4:4 + kbits], planes_hi[4:4 + kbits]):
                now = a & ~b
                less = now if less is None else now | (less & ~(a ^ b))
            if less is not None:
                better = better | (same & less)
        keep = ~better
        planes = [(a & keep) | (b & better) for a, b in zip(planes, planes_hi)] + [better]
        return [a | b for a, b in zip(have, have_hi)], planes

    for i in range(3):
        have, planes = fold(have, planes, lambda x: pltpu.roll(x, 8 - (1 << i), 0), True)
        where.append(4 + i)
    for i in range(log2(G)):
        have, planes = fold(have, planes, lambda x: pltpu.roll(x, 128 - (wd << i), 1), False)
        where.append(7 + kbits + i)

    have = [jnp.broadcast_to(x[0:1, :], (8, 128)) for x in have]
    planes = [jnp.broadcast_to(x[0:1, :], (8, 128)) for x in planes]
    for q in range(NI):
        idx = (sub + 8 * q) * 4 + lane // 32

        def bits(x):
            return lax.shift_right_logical(gather_lanes(x, idx), bit) & 1

        key = jnp.full((8, 128), (LEVELS + 1) * total, jnp.int32)
        for x in have:
            key = key - bits(x) * total
        parent = jnp.full((8, 128), me_r * height, jnp.int32)
        for p, x in zip(where, planes):
            parent = parent + (bits(x) << p)
        key_buf[0, q] = key + parent
    pend4 = exchange("row", R, me_r, key_buf, key_send, key_recv)
    for copy in pend4:
        copy.wait_recv()
    for q in range(NI):
        key = key_buf[0, q]
        for step in range(1, R):
            key = jnp.minimum(key, key_buf[step, q])
        seed, vid = seeds(q)
        key_ref[pl.ds(8 * q, 8), :] = jnp.where(seed, vid, key)
    for copy in pend1 + pend2 + pend3 + pend4:
        copy.wait_send()


def solution(mesh):
    R, C = mesh.shape["row"], mesh.shape["col"]

    def local(adjacency, seed_mask, source):
        height, wd = adjacency.shape
        width = seed_mask.shape[0]
        total = R * height
        G = 128 // wd
        NI = width // 1024
        NR = height // 1024
        vmem = pl.BlockSpec(memory_space=pltpu.VMEM)
        DMA = pltpu.SemaphoreType.DMA
        key = pl.pallas_call(
            functools.partial(kernel, R, C),
            out_shape=pltpu.VMEM((width // 128, 128), jnp.int32),
            in_specs=[pl.BlockSpec(memory_space=pl.ANY)] * 2 + [pl.BlockSpec(memory_space=pltpu.SMEM)],
            out_specs=vmem,
            scratch_shapes=[
                pltpu.VMEM((height // 128 * wd, 128), jnp.int32),
                DMA((height // 128,)),
                pltpu.VMEM((width // 128, 128), jnp.int32),
                DMA(()),
                pltpu.VMEM((128, 128), jnp.int32),
                pltpu.VMEM((height // 8 // G, 8, 128), jnp.int32),
                pltpu.VMEM((2, C, NR // 2, 8, 128), jnp.int32),
                pltpu.VMEM((R, NI, 8, 128), jnp.int32),
                pltpu.VMEM((R, NI, 8, 128), jnp.int32),
                DMA((2, C)), DMA((2, C)), DMA((R,)), DMA((R,)), DMA((R,)), DMA((R,)),
            ],
            compiler_params=pltpu.CompilerParams(collective_id=0, has_side_effects=True),
        )(adjacency.T, seed_mask.reshape(width // 128, 128), source)
        key = key.reshape(width)
        level = jnp.zeros_like(key)
        for d in range(1, LEVELS + 1):
            level = level + (key >= d * total).astype(jnp.int32)
        none = key >= (LEVELS + 1) * total
        return jnp.where(none, -1, level), jnp.where(none, -1, key - level * total)

    in_specs = (P("row", "col"), P("col"), P())
    out_specs = (P("col"), P("col"))
    return jax.shard_map(local, mesh=mesh, in_specs=in_specs, out_specs=out_specs, check_vma=False)
```

```python
import functools

import jax
import jax.numpy as jnp
from jax import lax
from jax.experimental import pallas as pl
from jax.experimental.pallas import tpu as pltpu
from jax.sharding import PartitionSpec as P

LEVELS = 4
MESH = pl.DeviceIdType.MESH
PAIR = 0x10001


def log2(n):
    return n.bit_length() - 1


def gather_lanes(x, idx):
    return jnp.take_along_axis(x, idx, axis=1)


def far_first(count):
    return sorted(range(1, count), key=lambda s: -min(s, count - s))


def any_of(values):
    values = list(values)
    while len(values) > 1:
        pairs = [values[i] | values[i + 1] for i in range(0, len(values) - 1, 2)]
        values = pairs + values[len(pairs) * 2:]
    return values[0]


def repeat(n, body, init):
    if n <= 4:
        for i in range(n):
            init = body(i, init)
        return init
    return lax.fori_loop(0, n, body, init)


def merge(low, high):
    rest = ~low[0]
    out = [low[0] | high[0]]
    for a, b in zip(low[1:], high[1:]):
        out.append(a | (b & rest))
    out.append(high[0] & rest)
    return out


def kernel(R, C, hbm_ref, seed_hbm, src_ref, key_ref,
           adj_ref, load_sem, seed_ref, small_sem, turn_ref, words_ref, col_buf, row_buf, key_buf,
           col_send, col_recv, row_send, row_recv, key_send, key_recv):
    me_r = lax.axis_index("row")
    me_c = lax.axis_index("col")
    barrier = pltpu.get_barrier_semaphore()
    for step in far_first(C):
        pl.semaphore_signal(barrier, inc=1, device_id={"col": lax.rem(me_c + step, C)}, device_id_type=MESH)
    for step in far_first(R):
        pl.semaphore_signal(barrier, inc=1, device_id={"row": lax.rem(me_r + step, R)}, device_id_type=MESH)

    wd, height = hbm_ref.shape
    small = pltpu.make_async_copy(seed_hbm, seed_ref, small_sem)
    loads = [pltpu.make_async_copy(hbm_ref.at[:, pl.ds(128 * t, 128)], adj_ref.at[pl.ds(wd * t, wd), :], load_sem.at[t])
             for t in range(height // 128)]
    for load in [small] + loads:
        load.start()
    G = 128 // wd
    NI = wd // 32
    NR = height // 1024
    NK = height // 128 // G
    owners = NR // NI
    total = R * height

    lane = lax.broadcasted_iota(jnp.int32, (8, 128), 1)
    sub = lax.broadcasted_iota(jnp.int32, (8, 128), 0)
    bit = lane % 32
    zero = jnp.zeros((8, 128), jnp.int32)
    small.wait()
    source = src_ref[0]
    first = me_c * (wd * 32)

    def seeds(q):
        vid = first + (sub + 8 * q) * 128 + lane
        return (seed_ref[pl.ds(8 * q, 8), :] > 0) | (vid == source), vid

    def block(a, q, t):
        return adj_ref[pl.ds(wd * t + 32 * a + q, 8, stride=4), :]

    def pull(col_set):
        words = []
        for tile in col_set:
            x = tile << bit
            for sh in (1, 2, 4, 8, 16):
                x = x | pltpu.roll(x, 128 - sh, 1)
            words.append([gather_lanes(x, zero + 32 * q) for q in range(4)])
        codes = []
        for h in range(NR):
            accs = [any_of(block(a, q, 8 * h + t) & words[a][q] for a in range(NI) for q in range(4))
                    for t in range(8)]
            for sh in (4, 2, 1):
                low = (sub // sh) % 2 == 0
                half = []
                for t in range(sh):
                    keep = jnp.where(low, accs[t], accs[t + sh])
                    give = jnp.where(low, accs[t + sh], accs[t])
                    if sh == 4:
                        other = pltpu.roll(give, 4, 0)
                    else:
                        other = jnp.where(low, pltpu.roll(give, 8 - sh, 0), pltpu.roll(give, sh, 0))
                    half.append(keep | other)
                accs = half
            code = jnp.where(accs[0] != 0, 1, 0)
            own = me_c == me_r * owners + h // NI
            codes.append(code | jnp.where(own, 3 * col_set[h % NI], 0))
        return [codes[h] | (codes[h + NR // 2] << 16) for h in range(NR // 2)]

    def push(row_set):
        out = [[zero] * 4 for _ in range(NI)]
        for t in range(8 * NR):
            mask = jnp.broadcast_to(row_set[t // 8][t % 8:t % 8 + 1, :], (8, 128))
            for a in range(NI):
                for q in range(4):
                    out[a][q] = out[a][q] | (block(a, q, t) & mask)
        result = []
        for a in range(NI):
            parts = out[a]
            for sh in (64, 32):
                low = (lane // sh) % 2 == 0
                half = []
                for q in range(sh // 32):
                    keep = jnp.where(low, parts[q], parts[q + sh // 32])
                    give = jnp.where(low, parts[q + sh // 32], parts[q])
                    half.append(keep | gather_lanes(give, lane ^ sh))
                parts = half
            x = parts[0]
            for sh in (1, 2, 4, 8, 16):
                x = x | gather_lanes(x, lane ^ sh)
            value = lax.shift_right_logical(x, bit) & 1
            for o in range(owners):
                own = me_c == me_r * owners + o
                value = value | jnp.where(own, row_set[o * NI + a] & 1, 0)
            result.append(value)
        return result

    def exchange(axis, count, me, slot, send, recv):
        copies = []
        for step in far_first(count):
            copy = pltpu.make_async_remote_copy(
                src_ref=slot.at[0], dst_ref=slot.at[step],
                send_sem=send.at[step], recv_sem=recv.at[step],
                device_id={axis: lax.rem(me + step, count)}, device_id_type=MESH)
            copy.start()
            copies.append(copy)
        return copies

    def join_col(slot, copies):
        for copy in copies:
            copy.wait_recv()
        pairs = [any_of(slot[step, t] for step in range(C)) for t in range(NR // 2)]
        codes = pairs + [x >> 16 for x in pairs]
        return [(x << 31) >> 31 for x in codes], [(x << 30) >> 31 for x in codes]

    def turn():
        def step(k, carry):
            parts = [adj_ref[pl.ds(pl.multiple_of((NK * g + k) * wd, 8), wd), :] for g in range(G)]
            x = parts[0] if G == 1 else jnp.concatenate(parts, axis=0)
            turn_ref[...] = x.T
            for j in range(16):
                words_ref[k * 16 + j] = turn_ref[pl.ds(j, 8, stride=16), :]
            return carry

        repeat(NK, step, 0)

    def row_words(nxt, now):
        at = lane % 16
        for h in range(NR):
            x = ((nxt[h] & 1) << at) | ((now[h] & 1) << (at + 16))
            for sh in (1, 2, 4, 8):
                x = x | pltpu.roll(x, 128 - sh, 1)
            turn_ref[pl.ds(8 * h, 8), :] = x

    def tournaments(nxt, now):
        kbits = log2(NK)
        row_words(nxt, now)

        def step(k, carries):
            f = zero
            for g in range(G):
                row = jnp.broadcast_to(turn_ref[pl.ds(NK * g + k, 1), :], (8, 128))
                f = jnp.where(lane // wd == g, gather_lanes(row, sub * 16), f)
            leaves = [words_ref[k * 16 + j] for j in range(16)]
            outs = []
            for top, carry in zip((15, 31), carries):
                nodes = [[leaves[j] & ((f << (top - j)) >> 31)] for j in range(16)]
                while len(nodes) > 1:
                    nodes = [merge(nodes[i], nodes[i + 1]) for i in range(0, len(nodes), 2)]
                node = nodes[0]
                rest = ~carry[0]
                fresh = node[0] & rest
                out = [carry[0] | node[0]]
                for p in range(4):
                    out.append(carry[1 + p] | (node[1 + p] & rest))
                for p in range(kbits):
                    out.append(carry[5 + p] | (fresh & -((k >> p) & 1)))
                outs.append(tuple(out))
            return tuple(outs)

        return list(repeat(NK, step, ((zero,) * (5 + kbits),) * 2))

    for load in loads:
        load.wait()
    for t, tile in enumerate(pull([jnp.where(seeds(q)[0], 1, 0) for q in range(NI)])):
        col_buf[0, 0, t] = tile
    pl.semaphore_wait(barrier, R + C - 2)
    pend1 = exchange("col", C, me_c, col_buf.at[0], col_send.at[0], col_recv.at[0])
    turn()
    s1, s0 = join_col(col_buf.at[0], pend1)

    for t, tile in enumerate(push(s1)):
        row_buf[0, t] = tile
    pend2 = exchange("row", R, me_r, row_buf, row_send, row_recv)
    first_two = tournaments(s1, s0)
    for copy in pend2:
        copy.wait_recv()
    col_set = [any_of(row_buf[step, t] for step in range(R)) for t in range(NI)]

    for t, tile in enumerate(pull(col_set)):
        col_buf[1, 0, t] = tile
    pend3 = exchange("col", C, me_c, col_buf.at[1], col_send.at[1], col_recv.at[1])
    s3, s2 = join_col(col_buf.at[1], pend3)

    nodes = first_two + tournaments(s3, s2)
    have = [node[0] for node in nodes]
    planes = list(nodes[0][1:])
    for d in range(1, LEVELS):
        fresh = have[d] & ~have[d - 1]
        planes = [p | (q & fresh) for p, q in zip(planes, nodes[d][1:])]
    kbits = log2(NK)
    where = list(range(4)) + [7 + p for p in range(kbits)]

    def fold(have, planes, turned, by_step):
        have_hi = [turned(x) for x in have]
        planes_hi = [turned(x) for x in planes]
        better = any_of(b & ~a for a, b in zip(have, have_hi))
        if by_step:
            same = ~any_of(a ^ b for a, b in zip(have, have_hi))
            less = None
            for a, b in zip(planes[4:4 + kbits], planes_hi[4:4 + kbits]):
                now = a & ~b
                less = now if less is None else now | (less & ~(a ^ b))
            if less is not None:
                better = better | (same & less)
        keep = ~better
        planes = [(a & keep) | (b & better) for a, b in zip(planes, planes_hi)] + [better]
        return [a | b for a, b in zip(have, have_hi)], planes

    for i in range(3):
        have, planes = fold(have, planes, lambda x: pltpu.roll(x, 8 - (1 << i), 0), True)
        where.append(4 + i)
    for i in range(log2(G)):
        have, planes = fold(have, planes, lambda x: pltpu.roll(x, 128 - (wd << i), 1), False)
        where.append(7 + kbits + i)

    have = [jnp.broadcast_to(x[0:1, :], (8, 128)) for x in have]
    planes = [jnp.broadcast_to(x[0:1, :], (8, 128)) for x in planes]
    for q in range(NI):
        idx = (sub + 8 * q) * 4 + lane // 32

        def bits(x):
            return lax.shift_right_logical(gather_lanes(x, idx), bit) & 1

        key = jnp.full((8, 128), (LEVELS + 1) * total, jnp.int32)
        for x in have:
            key = key - bits(x) * total
        parent = jnp.full((8, 128), me_r * height, jnp.int32)
        for p, x in zip(where, planes):
            parent = parent + (bits(x) << p)
        key_buf[0, q] = key + parent
    pend4 = exchange("row", R, me_r, key_buf, key_send, key_recv)
    for copy in pend1 + pend2 + pend3:
        copy.wait_send()
    for copy in pend4:
        copy.wait_recv()
    for q in range(NI):
        key = key_buf[0, q]
        for step in range(1, R):
            key = jnp.minimum(key, key_buf[step, q])
        seed, vid = seeds(q)
        key_ref[pl.ds(8 * q, 8), :] = jnp.where(seed, vid, key)
    for copy in pend4:
        copy.wait_send()


def solution(mesh):
    R, C = mesh.shape["row"], mesh.shape["col"]

    def local(adjacency, seed_mask, source):
        height, wd = adjacency.shape
        width = seed_mask.shape[0]
        total = R * height
        G = 128 // wd
        NI = width // 1024
        NR = height // 1024
        vmem = pl.BlockSpec(memory_space=pltpu.VMEM)
        DMA = pltpu.SemaphoreType.DMA
        key = pl.pallas_call(
            functools.partial(kernel, R, C),
            out_shape=pltpu.VMEM((width // 128, 128), jnp.int32),
            in_specs=[pl.BlockSpec(memory_space=pl.ANY)] * 2 + [pl.BlockSpec(memory_space=pltpu.SMEM)],
            out_specs=vmem,
            scratch_shapes=[
                pltpu.VMEM((height // 128 * wd, 128), jnp.int32),
                DMA((height // 128,)),
                pltpu.VMEM((width // 128, 128), jnp.int32),
                DMA(()),
                pltpu.VMEM((128, 128), jnp.int32),
                pltpu.VMEM((height // 8 // G, 8, 128), jnp.int32),
                pltpu.VMEM((2, C, NR // 2, 8, 128), jnp.int32),
                pltpu.VMEM((R, NI, 8, 128), jnp.int32),
                pltpu.VMEM((R, NI, 8, 128), jnp.int32),
                DMA((2, C)), DMA((2, C)), DMA((R,)), DMA((R,)), DMA((R,)), DMA((R,)),
            ],
            compiler_params=pltpu.CompilerParams(collective_id=0, has_side_effects=True),
        )(adjacency.T, seed_mask.reshape(width // 128, 128), source)
        key = key.reshape(width)
        level = jnp.zeros_like(key)
        for d in range(1, LEVELS + 1):
            level = level + (key >= d * total).astype(jnp.int32)
        none = key >= (LEVELS + 1) * total
        return jnp.where(none, -1, level), jnp.where(none, -1, key - level * total)

    in_specs = (P("row", "col"), P("col"), P())
    out_specs = (P("col"), P("col"))
    return jax.shard_map(local, mesh=mesh, in_specs=in_specs, out_specs=out_specs, check_vma=False)
```
